32 devices in a mesh: ta: 2 (over core), gx: 16 (over z, y, x).
Axes of the slice: x: 2, y: 2, z: 4, core: 2. Of those that a mesh axis runs over, the one named last changes fastest.
Arguments:
- time_links: float32 [6, 2, 3, 3, 96, 4608], P('ta', None, None, None, 'gx'), may hold values from -1 to 1, as said below
Outputs:
- loop_planes: float32 [96, 2, 4608], P('gx', None, 'ta')
- correlator: float32 [96, 49], P('gx')
The draws below stay inside these ranges and needn't reach their ends.
Inputs may be any that keep to these rules, and one draw needn't show every extreme that they name: At every site and time, the matrix time_links[t, 0] + i time_links[t, 1] is special unitary.
All inputs are finite; a program needn't handle non-finite values.
Results may differ from the reference program's by a relative error of at most 0.00029.
Values sent between devices are 32-bit elements; how exact they have to be, the bound alone decides.
A program may use at most 64 MiB of HBM per device.

```python
import jax
import jax.numpy as jnp
from jax import lax

NY = 48
NZ = 96
NT = 6
NX = 96
RMAX = 48


def normalize(column_real, column_imag):
    inverse = lax.rsqrt(jnp.sum(column_real * column_real + column_imag * column_imag, axis=0) + 1e-20)
    return (column_real * inverse, column_imag * inverse)


def project(base_real, base_imag, column_real, column_imag):
    inner_real = jnp.sum(base_real * column_real + base_imag * column_imag, axis=0)
    inner_imag = jnp.sum(base_real * column_imag - base_imag * column_real, axis=0)
    new_real = column_real - (base_real * inner_real - base_imag * inner_imag)
    new_imag = column_imag - (base_real * inner_imag + base_imag * inner_real)
    return (new_real, new_imag)


def times_complex(first_real, first_imag, second_real, second_imag):
    return (first_real * second_real - first_imag * second_imag, first_real * second_imag + first_imag * second_real)


def along_planes(innovation, rate):
    keep = jnp.sqrt(1.0 - rate * rate)

    def advance(state, fresh):
        following = rate * state + keep * fresh
        return (following, following)
    first = innovation[0]
    _, rest = lax.scan(advance, first, innovation[1:])
    return jnp.concatenate([first[None], rest], axis=0)


def draw_time_links(key, part):
    base_key = jax.random.fold_in(key, 17)
    noise_key, scale_key, field_key, rate_key, amp_key, white_key = jax.random.split(base_key, 6)
    plane_sites = NY * NZ
    site_shape = (NT, NX, plane_sites)
    noise = jax.random.truncated_normal(noise_key, -4.0, 4.0, (2, 3, 3) + site_shape, jnp.float32)
    innovation = jax.random.truncated_normal(field_key, -4.0, 4.0, (NX, 2, plane_sites), jnp.float32)
    white = jax.random.truncated_normal(white_key, -4.0, 4.0, (2,) + site_shape, jnp.float32)
    strength = jax.random.uniform(scale_key, site_shape, jnp.float32, 4.0, 12.0)
    log_length = jax.random.uniform(rate_key, (plane_sites,), jnp.float32, 0.0, jnp.log(1.0 * NX))
    amplitude = jnp.exp(jax.random.uniform(amp_key, (plane_sites,), jnp.float32, jnp.log(0.4), jnp.log(1.2)))
    rate = jnp.exp(-jnp.exp(-log_length))
    field = along_planes(innovation, rate)
    phase_one = (amplitude * field[:, 0] / NT)[None] + 0.15 * white[0]
    phase_two = (amplitude * field[:, 1] / NT)[None] + 0.15 * white[1]
    phase_three = -(phase_one + phase_two)
    cos_rows = jnp.stack([jnp.cos(phase_one), jnp.cos(phase_two), jnp.cos(phase_three)])
    sin_rows = jnp.stack([jnp.sin(phase_one), jnp.sin(phase_two), jnp.sin(phase_three)])
    unit_matrix = jnp.eye(3, dtype=noise.dtype)[:, :, None, None, None]
    matrix_real = noise[0] + strength[None, None] * unit_matrix * cos_rows[:, None]
    matrix_imag = noise[1] + strength[None, None] * unit_matrix * sin_rows[:, None]
    first_real, first_imag = normalize(matrix_real[:, 0], matrix_imag[:, 0])
    second_real, second_imag = project(first_real, first_imag, matrix_real[:, 1], matrix_imag[:, 1])
    second_real, second_imag = normalize(second_real, second_imag)
    third_real, third_imag = project(first_real, first_imag, matrix_real[:, 2], matrix_imag[:, 2])
    third_real, third_imag = project(second_real, second_imag, third_real, third_imag)
    third_real, third_imag = normalize(third_real, third_imag)
    cross_real = []
    cross_imag = []
    for row_index in range(3):
        next_row = (row_index + 1) % 3
        last_row = (row_index + 2) % 3
        plus_real, plus_imag = times_complex(second_real[next_row], second_imag[next_row], third_real[last_row], third_imag[last_row])
        minus_real, minus_imag = times_complex(second_real[last_row], second_imag[last_row], third_real[next_row], third_imag[next_row])
        cross_real.append(plus_real - minus_real)
        cross_imag.append(plus_imag - minus_imag)
    det_real = jnp.zeros_like(cross_real[0])
    det_imag = jnp.zeros_like(cross_real[0])
    for row_index in range(3):
        term_real, term_imag = times_complex(first_real[row_index], first_imag[row_index], cross_real[row_index], cross_imag[row_index])
        det_real = det_real + term_real
        det_imag = det_imag + term_imag
    fixed_real, fixed_imag = times_complex(third_real, third_imag, det_real, -det_imag)
    whole_real = jnp.stack([first_real, second_real, fixed_real], axis=1)
    whole_imag = jnp.stack([first_imag, second_imag, fixed_imag], axis=1)
    matrix = jnp.stack([whole_real, whole_imag])
    return jnp.transpose(matrix, (3, 0, 1, 2, 4, 5))


def setup_inputs(seed: int = 0) -> dict:
    keys = jax.random.split(jax.random.key(seed), 2)
    return {
        "time_links": draw_time_links(jax.random.fold_in(keys[1], 71), 0),
    }


def complex_mul(left, right):
    terms_real = []
    terms_imag = []
    for middle in range(3):
        left_real = left[0][:, middle:middle + 1]
        left_imag = left[1][:, middle:middle + 1]
        right_real = right[0][middle:middle + 1]
        right_imag = right[1][middle:middle + 1]
        terms_real.append(left_real * right_real - left_imag * right_imag)
        terms_imag.append(left_real * right_imag + left_imag * right_real)
    return jnp.stack([terms_real[0] + terms_real[1] + terms_real[2], terms_imag[0] + terms_imag[1] + terms_imag[2]])


def trace_third(matrix):
    return (matrix[:, 0, 0] + matrix[:, 1, 1] + matrix[:, 2, 2]) / 3.0


def reference(time_links):
    product = time_links[0]
    for slice_index in range(1, NT):
        product = complex_mul(product, time_links[slice_index])
    loop_planes = jnp.transpose(trace_third(product), (1, 0, 2))
    columns = []
    for offset in range(RMAX + 1):
        rolled = jnp.roll(loop_planes, -offset, axis=0)
        columns.append(jnp.sum(loop_planes * rolled, axis=(1, 2)) / (NY * NZ))
    return loop_planes, jnp.stack(columns, axis=1)
```

```python
import functools

import jax
import jax.numpy as jnp
from jax import lax
from jax.experimental import pallas as pl
from jax.experimental.pallas import tpu as pltpu
from jax.sharding import PartitionSpec as P

LANES = 128
SUBLANES = 8
PARTS = 2
REDUCERS = 2 * 2 * PARTS
MESH = pl.DeviceIdType.MESH


def scope(name):
    return jax.named_scope(name)


def cross_conj(first, second):
    row = []
    for k in range(3):
        a, b = (k + 1) % 3, (k + 2) % 3
        ar, ai = first[a]
        br, bi = first[b]
        cr, ci = second[a]
        dr, di = second[b]
        real = (ar * dr - ai * di) - (br * cr - bi * ci)
        imag = (br * ci + bi * cr) - (ar * di + ai * dr)
        row.append((real, imag))
    return row


def row_times(row, matrix):
    out = []
    for k in range(3):
        real = imag = None
        for m in range(3):
            ar, ai = row[m]
            br, bi = matrix[m][k]
            pr = ar * br - ai * bi
            pi = ar * bi + ai * br
            real = pr if real is None else real + pr
            imag = pi if imag is None else imag + pi
        out.append((real, imag))
    return out


def product_rows(load, slices):
    rows = [[load(0, r, c) for c in range(3)] for r in range(2)]
    for t in range(1, slices):
        matrix = [[load(t, r, c) for c in range(3)] for r in range(2)]
        matrix.append(cross_conj(matrix[0], matrix[1]))
        rows = [row_times(row, matrix) for row in rows]
    return rows


def trace_of_product(left, right):
    right = right + [cross_conj(right[0], right[1])]
    real = imag = None
    for i in range(3):
        for j in range(3):
            ar, ai = left[i][j]
            br, bi = right[j][i]
            pr = ar * br - ai * bi
            pi = ar * bi + ai * br
            real = pr if real is None else real + pr
            imag = pi if imag is None else imag + pi
    return real / 3.0, imag / 3.0


def lateness(g):
    return g % 2 + g // 2 % 2 + g // 4


def kernel(
    dims,
    x_ref,
    loop_ref,
    corr_ref,
    xin,
    psend,
    precv,
    held,
    tr,
    gath,
    gram,
    part,
    in_sem,
    s1,
    r1,
    s2,
    r2,
    s3,
    r3,
    ready,
    partner,
):
    slices, planes, sites, gx_n, tiles, longest = dims
    rows = planes * tiles
    slab = planes // 2
    wide = planes * gx_n
    lane_tiles = gram.shape[0]
    groups = -(-rows // SUBLANES)
    cut = groups // 2
    ta = lax.axis_index("ta")
    gx = lax.axis_index("gx")
    other = 1 - ta
    base = gx_n // 4
    step = gx_n // 2 // REDUCERS
    mine = (gx - base) // step
    is_reducer = jnp.logical_and(
        jnp.logical_and(ta == 1, gx >= base),
        jnp.logical_and((gx - base) % step == 0, gx < base + REDUCERS * step),
    )
    from_part = mine % 2
    from_core = mine // 2 % 2
    from_comp = mine // 4
    late = lateness(gx)

    def home(h, q, core):
        return base + (q * 4 + core * 2 + h) * step

    def in_copy(order, h):
        owner = other if order == 0 else ta
        return pltpu.make_async_copy(
            x_ref.at[:, pl.ds(0, 2), :, :, pl.ds((owner * PARTS + h) * tiles, tiles)],
            xin.at[order * PARTS + h],
            in_sem.at[order * PARTS + h],
        )

    for order in range(2):
        for h in range(PARTS):
            in_copy(order, h).start()

    barrier = pltpu.get_barrier_semaphore()

    def arrive(semaphore, core, j):
        pl.semaphore_signal(semaphore, inc=1, device_id={"ta": core, "gx": j}, device_id_type=MESH)

    @pl.when(ta == 1)
    def _():
        arrive(barrier, 0, gx)

    expected = jnp.where(ta == 0, 1, 0)
    for h in range(PARTS):
        for q in range(2):
            place = home(h, q, ta)
            sooner = lateness(place) <= late

            @pl.when(jnp.logical_not(sooner))
            def _():
                arrive(barrier, 1, place)

            counts = jnp.logical_and(sooner, place != gx)
            expected = expected + jnp.where(counts, 1, 0)

    @pl.when(is_reducer)
    def _():
        def greet(j, carry):
            @pl.when(jnp.logical_and(late <= lateness(j), j != gx))
            def _():
                arrive(barrier, from_core, j)

            return carry

        lax.fori_loop(0, gx_n, greet, 0)

    before = jnp.int32(0)
    for j in range(gx_n):
        before = before + jnp.where(lateness(j) < late, 1, 0)
    expected = expected + jnp.where(is_reducer, before, 0)
    with scope("barrier"):

        @pl.when(expected > 0)
        def _():
            pl.semaphore_wait(barrier, expected)

    @pl.when(ta == 0)
    def _():
        arrive(partner, 1, gx)

    @pl.when(is_reducer)
    def _():
        def reply(j, carry):
            @pl.when(lateness(j) < late)
            def _():
                arrive(ready.at[from_part * 2 + from_comp], from_core, j)

            return carry

        lax.fori_loop(0, gx_n, reply, 0)

    flat_in = xin.reshape(*xin.shape[:4], rows * 2, LANES)
    flat_send = psend.reshape(PARTS, 12, rows, LANES)
    flat_recv = precv.reshape(PARTS, 12, rows, LANES)
    flat_loop = loop_ref.reshape(PARTS, rows * 2, LANES)
    flat_tr = tr.reshape(PARTS, 2, rows, LANES)
    flat_gath = gath.reshape(gx_n * rows, LANES)

    def loader(slot, start):
        def load(t, r, c):
            return tuple(
                flat_in[slot, t, r, c, pl.ds(2 * start + q, SUBLANES, stride=2), :]
                for q in range(2)
            )

        return load

    def begin(g):
        return jnp.minimum(g * SUBLANES, rows - SUBLANES)

    def swap(h, p):
        span = pl.ds(0, cut * SUBLANES // 2) if p == 0 else pl.ds(cut * SUBLANES // 2, rows // 2 - cut * SUBLANES // 2)
        return pltpu.make_async_remote_copy(
            src_ref=psend.at[h, :, span],
            dst_ref=precv.at[h, :, span],
            send_sem=s1.at[h * 2 + p],
            recv_sem=r1.at[h * 2 + p],
            device_id={"ta": other, "gx": gx},
            device_id_type=MESH,
        )

    pieces = ((0, cut), (cut, groups))

    for h in range(PARTS):
        with scope(f"farwait{h}"):
            in_copy(0, h).wait()
        for p, (low, high) in enumerate(pieces):
            def far(g, carry, h=h):
                start = begin(g)
                product = product_rows(loader(h, start), slices)
                for r in range(2):
                    for k in range(3):
                        for q in range(2):
                            flat_send[h, (r * 3 + k) * 2 + q, pl.ds(start, SUBLANES), :] = product[r][k][q]
                return carry

            with scope(f"far{h}{p}"):
                lax.fori_loop(low, high, far, 0)
            if h == 0 and p == 0:
                @pl.when(ta == 1)
                def _():
                    with scope("partner"):
                        pl.semaphore_wait(partner, 1)
            swap(h, p).start()

    for h in range(PARTS):
        with scope(f"nearwait{h}"):
            in_copy(1, h).wait()

        def near(g, carry, h=h):
            start = begin(g)
            product = product_rows(loader(PARTS + h, start), slices)
            product.append(cross_conj(product[0], product[1]))
            for r in range(3):
                for k in range(3):
                    for q in range(2):
                        held[h, (r * 3 + k) * 2 + q, pl.ds(start, SUBLANES), :] = product[r][k][q]
            return carry

        with scope(f"near{h}"):
            lax.fori_loop(0, groups, near, 0)

    def scatter(h, q, place):
        return pltpu.make_async_remote_copy(
            src_ref=tr.at[h, q],
            dst_ref=gath.at[gx],
            send_sem=s2,
            recv_sem=r2,
            device_id={"ta": 1, "gx": place},
            device_id_type=MESH,
        )

    for h in range(PARTS):
        for p, (low, high) in enumerate(pieces):
            with scope(f"swapwait{h}{p}"):
                swap(h, p).wait_recv()

            def trace(g, carry, h=h):
                start = begin(g)
                ours = [
                    [
                        tuple(held[h, (r * 3 + k) * 2 + q, pl.ds(start, SUBLANES), :] for q in range(2))
                        for k in range(3)
                    ]
                    for r in range(3)
                ]
                theirs = [
                    [
                        tuple(flat_recv[h, (r * 3 + k) * 2 + q, pl.ds(start, SUBLANES), :] for q in range(2))
                        for k in range(3)
                    ]
                    for r in range(2)
                ]
                pair = trace_of_product(ours, theirs)
                for q in range(2):
                    flat_loop[h, pl.ds(2 * start + q, SUBLANES, stride=2), :] = pair[q]
                    flat_tr[h, q, pl.ds(start, SUBLANES), :] = pair[q]
                return carry

            with scope(f"trace{h}{p}"):
                lax.fori_loop(low, high, trace, 0)
        for q in range(2):
            place = home(h, q, ta)
            itself = jnp.logical_and(ta == 1, place == gx)

            @pl.when(lateness(place) > late)
            def _():
                with scope(f"ready{h}{q}"):
                    pl.semaphore_wait(ready.at[h * 2 + q], 1)

            @pl.when(jnp.logical_not(itself))
            def _():
                scatter(h, q, place).start()

            @pl.when(itself)
            def _():
                gath[gx] = tr[h, q]

    def report(core, j, slot):
        return pltpu.make_async_remote_copy(
            src_ref=gram.at[:, pl.ds(j * slab, slab)],
            dst_ref=part.at[slot],
            send_sem=s3,
            recv_sem=r3,
            device_id={"ta": core, "gx": j},
            device_id_type=MESH,
        )

    def total(ref, semaphore):
        return pltpu.make_async_copy(ref, ref, semaphore)

    @pl.when(is_reducer)
    def _():
        with scope("gather"):
            @pl.when(from_core == 0)
            def _():
                total(gath, r2).wait()

            @pl.when(from_core == 1)
            def _():
                total(gath.at[pl.ds(0, gx_n - 1)], r2).wait()

        with scope("gram"):
            highs, lows = [], []
            for i in range(tiles):
                values = flat_gath[pl.ds(i, wide, stride=tiles), :]
                high = values.astype(jnp.bfloat16)
                highs.append(high)
                lows.append((values - high.astype(jnp.float32)).astype(jnp.bfloat16))
            high = jnp.concatenate(highs, axis=1)
            low = jnp.concatenate(lows, axis=1)

            def dot(a, b):
                return lax.dot_general(a, b, (((1,), (1,)), ((), ())), preferred_element_type=jnp.float32)

            product = dot(high, high) + (dot(high, low) + dot(low, high))
            padding = lane_tiles * LANES - wide
            if padding:
                product = jnp.concatenate([product, jnp.zeros((wide, padding), jnp.float32)], axis=1)
            flat_gram = gram.reshape(lane_tiles, wide, LANES)
            for i in range(lane_tiles):
                flat_gram[i] = product[:, i * LANES : (i + 1) * LANES]
        with scope("report"):
            for core in range(2):

                def tell(j, carry, core=core):
                    @pl.when(jnp.logical_or(core != ta, j != gx))
                    def _():
                        report(core, j, mine).start()

                    return carry

                lax.fori_loop(0, gx_n, tell, 0)
            part[mine] = gram[:, pl.ds(gx * slab, slab)]
        with scope("hear_r"):
            total(part.at[pl.ds(0, REDUCERS - 1)], r3).wait()

    @pl.when(jnp.logical_not(is_reducer))
    def _():
        with scope("hear"):
            total(part, r3).wait()

    sc = scope("final")
    sc.__enter__()
    flat_part = part.reshape(REDUCERS, lane_tiles, planes, LANES)
    chunks = []
    for i in range(lane_tiles):
        chunk = flat_part[0, i]
        for slot in range(1, REDUCERS):
            chunk = chunk + flat_part[slot, i]
        chunks.append(chunk)
    summed = chunks[0] if lane_tiles == 1 else jnp.concatenate(chunks, axis=1)
    extra = -planes % SUBLANES
    if extra:
        summed = jnp.concatenate([summed, jnp.zeros((extra, summed.shape[1]), jnp.float32)], axis=0)
    width = summed.shape[1]
    row_index = lax.broadcasted_iota(jnp.int32, summed.shape, 0)
    column = lax.broadcasted_iota(jnp.int32, summed.shape, 1)
    answer = jnp.zeros(summed.shape, jnp.float32)
    for i in range(planes):
        start = gx * planes + i
        ahead = pltpu.roll(summed, (width - start) % width, 1)
        if width == wide:
            value = ahead
        else:
            around = pltpu.roll(summed, (width + wide - start) % width, 1)
            value = jnp.where(column + start < wide, ahead, around)
        answer = jnp.where(row_index == i, value, answer)
    corr_ref[...] = answer[0:planes, 0 : longest + 1] / sites
    sc.__exit__(None, None, None)

    sc = scope("drain")
    sc.__enter__()
    for h in range(PARTS):
        for p in range(2):
            swap(h, p).wait_send()

    inside = jnp.logical_and(is_reducer, from_core == 1)
    sent = tr.reshape(PARTS * 2, rows // 2, 2, LANES)

    @pl.when(inside)
    def _():
        total(sent.at[pl.ds(0, 3)], s2).wait()

    @pl.when(jnp.logical_not(inside))
    def _():
        total(sent, s2).wait()

    @pl.when(is_reducer)
    def _():
        count = (2 * gx_n - 1) * slab * lane_tiles
        total(gath.reshape(gx_n * rows // 2, 2, LANES).at[pl.ds(0, count)], s3).wait()

    sc.__exit__(None, None, None)


def place_outputs(loop_in, corr_in, loop_out, corr_out, semaphores):
    tiles = loop_in.shape[2]
    copies = [pltpu.make_async_copy(corr_in, corr_out, semaphores.at[PARTS])]
    for h in range(PARTS):
        copies.append(
            pltpu.make_async_copy(
                loop_in.at[h], loop_out.at[:, pl.ds(h * tiles, tiles)], semaphores.at[h]
            )
        )
    for copy in copies:
        copy.start()
    for copy in copies:
        copy.wait()


def per_device(gx_n, time_links):
    slices, _, _, _, planes, sites = time_links.shape
    blocks = sites // LANES
    held = time_links.transpose(0, 2, 3, 4, 1, 5)
    held = held.reshape(slices, 3, 3, planes, 2, blocks, LANES).swapaxes(4, 5)
    tiles = blocks // 2 // PARTS
    rows = planes * tiles
    longest = planes * (gx_n // 2)
    wide = planes * gx_n
    lane_tiles = -(-wide // LANES)
    dims = (slices, planes, sites, gx_n, tiles, longest)
    dma = pltpu.SemaphoreType.DMA
    f32 = jnp.float32
    loops, correlator = pl.pallas_call(
        functools.partial(kernel, dims),
        out_shape=(
            pltpu.VMEM((PARTS, planes, tiles, 2, LANES), f32),
            pltpu.VMEM((planes, longest + 1), f32),
        ),
        in_specs=[pl.BlockSpec(memory_space=pl.ANY)],
        out_specs=(
            pl.BlockSpec(memory_space=pltpu.VMEM),
            pl.BlockSpec(memory_space=pltpu.VMEM),
        ),
        scratch_shapes=[
            pltpu.VMEM((2 * PARTS, slices, 2, 3, planes, tiles, 2, LANES), f32),
            pltpu.VMEM((PARTS, 12, rows // 2, 2, LANES), f32),
            pltpu.VMEM((PARTS, 12, rows // 2, 2, LANES), f32),
            pltpu.VMEM((PARTS, 18, rows, LANES), f32),
            pltpu.VMEM((PARTS, 2, rows // 2, 2, LANES), f32),
            pltpu.VMEM((gx_n, rows // 2, 2, LANES), f32),
            pltpu.VMEM((lane_tiles, wide // 2, 2, LANES), f32),
            pltpu.VMEM((REDUCERS, lane_tiles, planes // 2, 2, LANES), f32),
            dma((2 * PARTS,)),
            dma((2 * PARTS,)),
            dma((2 * PARTS,)),
            dma,
            dma,
            dma,
            dma,
            pltpu.SemaphoreType.REGULAR((2 * PARTS,)),
            pltpu.SemaphoreType.REGULAR,
        ],
        compiler_params=pltpu.CompilerParams(collective_id=0, has_side_effects=True),
    )(held)
    loops = pltpu.with_memory_space_constraint(loops, pltpu.VMEM)
    correlator = pltpu.with_memory_space_constraint(correlator, pltpu.VMEM)
    loops, correlator = pl.pallas_call(
        place_outputs,
        out_shape=(
            jax.ShapeDtypeStruct((planes, blocks // 2, 2, LANES), f32),
            jax.ShapeDtypeStruct((planes, longest + 1), f32),
        ),
        in_specs=[pl.BlockSpec(memory_space=pltpu.VMEM)] * 2,
        out_specs=(pl.BlockSpec(memory_space=pl.ANY),) * 2,
        scratch_shapes=[dma((PARTS + 1,))],
    )(loops, correlator)
    return loops.swapaxes(1, 2).reshape(planes, 2, sites // 2), correlator


def solution(mesh):
    in_specs = (P("ta", None, None, None, "gx", None),)
    out_specs = (P("gx", None, "ta"), P("gx", None))
    return jax.shard_map(
        functools.partial(per_device, mesh.shape["gx"]),
        mesh=mesh,
        in_specs=in_specs,
        out_specs=out_specs,
        check_vma=False,
    )
```

```python
import functools

import jax
import jax.numpy as jnp
from jax import lax
from jax.experimental import pallas as pl
from jax.experimental.pallas import tpu as pltpu
from jax.sharding import PartitionSpec as P

LANES = 128
SUBLANES = 8
PARTS = 2
REDUCERS = 2 * 2 * PARTS
MESH = pl.DeviceIdType.MESH


def scope(name):
    return jax.named_scope(name)


def cross_conj(first, second):
    row = []
    for k in range(3):
        a, b = (k + 1) % 3, (k + 2) % 3
        ar, ai = first[a]
        br, bi = first[b]
        cr, ci = second[a]
        dr, di = second[b]
        real = (ar * dr - ai * di) - (br * cr - bi * ci)
        imag = (br * ci + bi * cr) - (ar * di + ai * dr)
        row.append((real, imag))
    return row


def row_times(row, matrix):
    out = []
    for k in range(3):
        real = imag = None
        for m in range(3):
            ar, ai = row[m]
            br, bi = matrix[m][k]
            pr = ar * br - ai * bi
            pi = ar * bi + ai * br
            real = pr if real is None else real + pr
            imag = pi if imag is None else imag + pi
        out.append((real, imag))
    return out


def product_rows(load, slices):
    rows = [[load(0, r, c) for c in range(3)] for r in range(2)]
    for t in range(1, slices):
        matrix = [[load(t, r, c) for c in range(3)] for r in range(2)]
        matrix.append(cross_conj(matrix[0], matrix[1]))
        rows = [row_times(row, matrix) for row in rows]
    return rows


def trace_of_product(left, right):
    right = right + [cross_conj(right[0], right[1])]
    real = imag = None
    for i in range(3):
        for j in range(3):
            ar, ai = left[i][j]
            br, bi = right[j][i]
            pr = ar * br - ai * bi
            pi = ar * bi + ai * br
            real = pr if real is None else real + pr
            imag = pi if imag is None else imag + pi
    return real / 3.0, imag / 3.0


def kernel(dims, split, x_ref, *refs):
    slices, planes, sites, gx_n, longest = dims
    count = len(split)
    refs = list(refs)

    def take(n):
        taken = refs[:n]
        del refs[:n]
        return taken

    loop_refs = take(count)
    (corr_ref,) = take(1)
    far_in, near_in = take(count), take(count)
    psend, precv, held, tr = take(count), take(count), take(count), take(count)
    gath = take(2)
    gram, part, in_sem, s1, r1, s2, r2, s3, r3, ready, partner, cleared = refs
    slab = planes // 2
    wide = planes * gx_n
    lane_tiles = gram.shape[0]
    ta = lax.axis_index("ta")
    gx = lax.axis_index("gx")
    other = 1 - ta
    half = sum(n for _, n in split)
    base = gx_n // 4
    step = gx_n // 2 // REDUCERS
    mine = (gx - base) // step
    is_home = jnp.logical_and(
        gx >= base,
        jnp.logical_and((gx - base) % step == 0, gx < base + REDUCERS * step),
    )
    is_reducer = jnp.logical_and(ta == 1, is_home)
    from_part = mine % 2
    from_core = mine // 2 % 2
    from_comp = mine // 4
    early = gx_n // 2 + gx_n // 4
    near_targets = gx_n // 4
    is_first = gx == 0

    def home(h, q, core):
        return base + (q * 4 + core * 2 + h) * step

    def in_copy(order, p):
        owner = other if order == 0 else ta
        start, n = split[p]
        return pltpu.make_async_copy(
            x_ref.at[:, pl.ds(0, 2), :, :, pl.ds(owner * half + start, n)],
            (far_in, near_in)[order][p],
            in_sem.at[order * count + p],
        )

    for order in range(2):
        for p in range(count):
            in_copy(order, p).start()

    barrier = pltpu.get_barrier_semaphore()

    def arrive(semaphore, core, j):
        pl.semaphore_signal(semaphore, inc=1, device_id={"ta": core, "gx": j}, device_id_type=MESH)

    @pl.when(ta == 1)
    def _():
        arrive(barrier, 0, gx)

    @pl.when(is_first)
    def _():
        for h in range(PARTS):
            for q in range(2):
                arrive(barrier, 0, home(h, q, ta))

    @pl.when(is_reducer)
    def _():
        for j in range(1, gx_n):

            @pl.when(j != gx)
            def _():
                arrive(barrier, 1, j)

    @pl.when(ta == 0)
    def _():
        with scope("join"):
            pl.semaphore_wait(barrier, jnp.where(is_home, 2, 1))
        arrive(partner, 1, gx)

        @pl.when(is_home)
        def _():
            arrive(ready.at[from_part * 2 + from_comp], from_core, 0)

    def clear():
        @pl.when(jnp.logical_and(ta == 1, jnp.logical_not(is_first)))
        def _():
            pl.semaphore_wait(barrier, jnp.where(is_home, REDUCERS - 1, REDUCERS))
            arrive(cleared, 0, gx)

        @pl.when(jnp.logical_and(ta == 0, jnp.logical_not(is_first)))
        def _():
            pl.semaphore_wait(cleared, 1)

    def rows_of(p):
        return planes * split[p][1]

    def begin(p, g):
        return jnp.minimum(g * SUBLANES, rows_of(p) - SUBLANES)

    def each_group(p, body):
        def run(g, carry):
            body(begin(p, g))
            return carry

        lax.fori_loop(0, -(-rows_of(p) // SUBLANES), run, 0)

    def loader(ref, rows, start):
        flat = ref.reshape(*ref.shape[:3], rows * 2, LANES)

        def load(t, r, c):
            return tuple(
                flat[t, r, c, pl.ds(2 * start + q, SUBLANES, stride=2), :] for q in range(2)
            )

        return load

    def flat_rows(ref):
        return ref.reshape(ref.shape[0], ref.shape[1] * 2, LANES)

    def swap(p):
        return pltpu.make_async_remote_copy(
            src_ref=psend[p],
            dst_ref=precv[p],
            send_sem=s1.at[p],
            recv_sem=r1.at[p],
            device_id={"ta": other, "gx": gx},
            device_id_type=MESH,
        )

    for p in range(count):
        with scope(f"farwait{p}"):
            in_copy(0, p).wait()

        def far(start, p=p):
            product = product_rows(loader(far_in[p], rows_of(p), start), slices)
            out = flat_rows(psend[p])
            for r in range(2):
                for k in range(3):
                    for q in range(2):
                        out[(r * 3 + k) * 2 + q, pl.ds(start, SUBLANES), :] = product[r][k][q]

        with scope(f"far{p}"):
            each_group(p, far)
        if p == 0:

            @pl.when(ta == 1)
            def _():
                with scope("partner"):
                    pl.semaphore_wait(partner, 1)

        swap(p).start()

    for p in range(count):
        with scope(f"nearwait{p}"):
            in_copy(1, p).wait()

        def near(start, p=p):
            product = product_rows(loader(near_in[p], rows_of(p), start), slices)
            product.append(cross_conj(product[0], product[1]))
            for r in range(3):
                for k in range(3):
                    for q in range(2):
                        held[p][(r * 3 + k) * 2 + q, pl.ds(start, SUBLANES), :] = product[r][k][q]

        with scope(f"near{p}"):
            each_group(p, near)

    def scatter(p, q, place):
        return pltpu.make_async_remote_copy(
            src_ref=tr[p].at[q],
            dst_ref=gath[p % 2].at[gx],
            send_sem=s2,
            recv_sem=r2.at[jnp.where(gx < early, 0, 2) + p % 2],
            device_id={"ta": 1, "gx": place},
            device_id_type=MESH,
        )

    def hand_over(p, q):
        place = home(p // 2, q, ta)
        itself = jnp.logical_and(ta == 1, place == gx)

        @pl.when(jnp.logical_not(itself))
        def _():
            scatter(p, q, place).start()

        @pl.when(itself)
        def _():
            gath[p % 2][gx] = tr[p][q]

    upper = jnp.where(gx < gx_n // 2, 1, 0)

    for p in range(count):
        with scope(f"swapwait{p}"):
            swap(p).wait_recv()

        def trace(start, p=p):
            theirs_ref = flat_rows(precv[p])

            def entry(ref, r, k):
                return tuple(ref[(r * 3 + k) * 2 + q, pl.ds(start, SUBLANES), :] for q in range(2))

            ours = [[entry(held[p], r, k) for k in range(3)] for r in range(3)]
            theirs = [[entry(theirs_ref, r, k) for k in range(3)] for r in range(2)]
            pair = trace_of_product(ours, theirs)
            flat_loop = loop_refs[p].reshape(rows_of(p) * 2, LANES)
            flat_tr = flat_rows(tr[p])
            for q in range(2):
                flat_loop[pl.ds(2 * start + q, SUBLANES, stride=2), :] = pair[q]
                flat_tr[q, pl.ds(start, SUBLANES), :] = pair[q]

        with scope(f"trace{p}"):
            each_group(p, trace)
        if p == 0:
            with scope("clear"):
                clear()

        @pl.when(jnp.logical_not(is_first))
        def _():
            hand_over(p, upper)
            hand_over(p, 1 - upper)

    @pl.when(is_first)
    def _():
        for h in range(PARTS):
            for q in range(2):
                with scope(f"ready{h}{q}"):
                    pl.semaphore_wait(ready.at[h * 2 + q], 1)
                for k in range(2):
                    hand_over(h * 2 + k, q)

    def report(core, j, slot):
        return pltpu.make_async_remote_copy(
            src_ref=gram.at[:, pl.ds(j * slab, slab)],
            dst_ref=part.at[slot],
            send_sem=s3,
            recv_sem=r3,
            device_id={"ta": core, "gx": j},
            device_id_type=MESH,
        )

    def total(ref, semaphore):
        return pltpu.make_async_copy(ref, ref, semaphore)

    flat_gram = gram.reshape(lane_tiles, wide, LANES)

    def contract(k, low, high, width):
        tiles = split[k][1]
        flat_gath = gath[k].reshape(gx_n * rows_of(k), LANES)
        tops, bottoms = [], []
        for i in range(tiles):
            values = flat_gath[pl.ds(i, width, stride=tiles), :]
            top = values.astype(jnp.bfloat16)
            tops.append(top)
            bottoms.append((values - top.astype(jnp.float32)).astype(jnp.bfloat16))
        top = jnp.concatenate(tops, axis=1)
        bottom = jnp.concatenate(bottoms, axis=1)

        def dot(a, b):
            return lax.dot_general(a, b, (((1,), (1,)), ((), ())), preferred_element_type=jnp.float32)

        return dot(top[low:high], top) + (dot(top[low:high], bottom) + dot(bottom[low:high], top))

    def place_rows(product, low, high, width):
        padding = lane_tiles * LANES - width
        if padding:
            product = jnp.concatenate([product, jnp.zeros((high - low, padding), jnp.float32)], axis=1)
        for i in range(lane_tiles):
            flat_gram[i, low:high] = product[:, i * LANES : (i + 1) * LANES]

    def tell(j, carry):
        for core in range(2):

            @pl.when(jnp.logical_or(core != ta, j != gx))
            def _():
                report(core, j, mine).start()

        return carry

    @pl.when(is_reducer)
    def _():
        first_rows = planes * near_targets
        products = []
        for k in range(2):
            with scope(f"gather0{k}"):
                @pl.when(from_core == 0)
                def _():
                    total(gath[k].at[pl.ds(0, early)], r2.at[k]).wait()

                @pl.when(from_core == 1)
                def _():
                    total(gath[k].at[pl.ds(0, early - 1)], r2.at[k]).wait()

            with scope(f"gram0{k}"):
                products.append(contract(k, 0, first_rows, planes * early))
        place_rows(products[0] + products[1], 0, first_rows, planes * early)
        with scope("report0"):
            lax.fori_loop(0, near_targets, tell, 0)
        products = []
        for k in range(2):
            with scope(f"gather1{k}"):
                total(gath[k].at[pl.ds(0, gx_n - early)], r2.at[2 + k]).wait()
            with scope(f"gram1{k}"):
                products.append(contract(k, first_rows, wide, wide))
        place_rows(products[0] + products[1], first_rows, wide, wide)
        with scope("report1"):
            lax.fori_loop(near_targets, gx_n, tell, 0)
            part[mine] = gram[:, pl.ds(gx * slab, slab)]
        with scope("hear_r"):
            total(part.at[pl.ds(0, REDUCERS - 1)], r3).wait()

    @pl.when(jnp.logical_not(is_reducer))
    def _():
        with scope("hear"):
            total(part, r3).wait()

    sc = scope("final")
    sc.__enter__()
    flat_part = part.reshape(REDUCERS, lane_tiles, planes, LANES)
    chunks = []
    for i in range(lane_tiles):
        chunk = flat_part[0, i]
        for slot in range(1, REDUCERS):
            chunk = chunk + flat_part[slot, i]
        chunks.append(chunk)
    summed = chunks[0] if lane_tiles == 1 else jnp.concatenate(chunks, axis=1)
    extra = -planes % SUBLANES
    if extra:
        summed = jnp.concatenate([summed, jnp.zeros((extra, summed.shape[1]), jnp.float32)], axis=0)
    width = summed.shape[1]
    row_index = lax.broadcasted_iota(jnp.int32, summed.shape, 0)
    column = lax.broadcasted_iota(jnp.int32, summed.shape, 1)
    answer = jnp.zeros(summed.shape, jnp.float32)
    for i in range(planes):
        start = gx * planes + i
        ahead = pltpu.roll(summed, (width - start) % width, 1)
        if width == wide:
            value = ahead
        else:
            around = pltpu.roll(summed, (width + wide - start) % width, 1)
            value = jnp.where(column + start < wide, ahead, around)
        answer = jnp.where(row_index == i, value, answer)
    corr_ref[...] = answer[0:planes, 0 : longest + 1] / sites
    sc.__exit__(None, None, None)

    sc = scope("drain")
    sc.__enter__()
    for p in range(count):
        swap(p).wait_send()

    inside = jnp.logical_and(is_reducer, from_core == 1)
    pool = gath[1].reshape(gx_n * rows_of(1) // 2, 2, LANES)
    message = planes * half // PARTS // 2

    @pl.when(inside)
    def _():
        total(pool.at[pl.ds(0, 3 * message)], s2).wait()

    @pl.when(jnp.logical_not(inside))
    def _():
        total(pool.at[pl.ds(0, 4 * message)], s2).wait()

    @pl.when(is_reducer)
    def _():
        left = (2 * gx_n - 1) * slab * lane_tiles
        while left:
            length = min(left, pool.shape[0])
            total(pool.at[pl.ds(0, length)], s3).wait()
            left -= length

    sc.__exit__(None, None, None)


def place_outputs(split, *refs):
    count = len(split)
    loop_in, (corr_in, loop_out, corr_out, semaphores) = refs[:count], refs[count:]
    copies = [pltpu.make_async_copy(corr_in, corr_out, semaphores.at[count])]
    for p, (start, n) in enumerate(split):
        copies.append(
            pltpu.make_async_copy(loop_in[p], loop_out.at[:, pl.ds(start, n)], semaphores.at[p])
        )
    for copy in copies:
        copy.start()
    for copy in copies:
        copy.wait()


def per_device(gx_n, time_links):
    slices, _, _, _, planes, sites = time_links.shape
    blocks = sites // LANES
    held = time_links.transpose(0, 2, 3, 4, 1, 5)
    held = held.reshape(slices, 3, 3, planes, 2, blocks, LANES).swapaxes(4, 5)
    half = blocks // 2
    tiles = half // PARTS
    small = tiles // 2
    split = []
    for h in range(PARTS):
        split += [(h * tiles, small), (h * tiles + small, tiles - small)]
    longest = planes * (gx_n // 2)
    wide = planes * gx_n
    lane_tiles = -(-wide // LANES)
    dims = (slices, planes, sites, gx_n, longest)
    dma = pltpu.SemaphoreType.DMA
    regular = pltpu.SemaphoreType.REGULAR
    f32 = jnp.float32
    count = len(split)
    links = [pltpu.VMEM((slices, 2, 3, planes, n, 2, LANES), f32) for _, n in split]
    swaps = [pltpu.VMEM((12, planes * n // 2, 2, LANES), f32) for _, n in split]
    scratch = links + links + swaps + swaps
    scratch += [pltpu.VMEM((18, planes * n, LANES), f32) for _, n in split]
    scratch += [pltpu.VMEM((2, planes * n // 2, 2, LANES), f32) for _, n in split]
    scratch += [pltpu.VMEM((gx_n, planes * n // 2, 2, LANES), f32) for _, n in split[:2]]
    scratch += [
        pltpu.VMEM((lane_tiles, wide // 2, 2, LANES), f32),
        pltpu.VMEM((REDUCERS, lane_tiles, planes // 2, 2, LANES), f32),
        dma((2 * count,)),
        dma((count,)),
        dma((count,)),
        dma,
        dma((4,)),
        dma,
        dma,
        regular((2 * PARTS,)),
        regular,
        regular,
    ]
    in_vmem = pl.BlockSpec(memory_space=pltpu.VMEM)
    results = pl.pallas_call(
        functools.partial(kernel, dims, split),
        out_shape=[pltpu.VMEM((planes, n, 2, LANES), f32) for _, n in split]
        + [pltpu.VMEM((planes, longest + 1), f32)],
        in_specs=[pl.BlockSpec(memory_space=pl.ANY)],
        out_specs=[in_vmem] * (count + 1),
        scratch_shapes=scratch,
        compiler_params=pltpu.CompilerParams(collective_id=0, has_side_effects=True),
    )(held)
    results = [pltpu.with_memory_space_constraint(r, pltpu.VMEM) for r in results]
    loops, correlator = pl.pallas_call(
        functools.partial(place_outputs, split),
        out_shape=(
            jax.ShapeDtypeStruct((planes, half, 2, LANES), f32),
            jax.ShapeDtypeStruct((planes, longest + 1), f32),
        ),
        in_specs=[in_vmem] * (count + 1),
        out_specs=(pl.BlockSpec(memory_space=pl.ANY),) * 2,
        scratch_shapes=[dma((count + 1,))],
    )(*results)
    return loops.swapaxes(1, 2).reshape(planes, 2, sites // 2), correlator


def solution(mesh):
    in_specs = (P("ta", None, None, None, "gx", None),)
    out_specs = (P("gx", None, "ta"), P("gx", None))
    return jax.shard_map(
        functools.partial(per_device, mesh.shape["gx"]),
        mesh=mesh,
        in_specs=in_specs,
        out_specs=out_specs,
        check_vma=False,
    )
```

```python
import functools

import jax
import jax.numpy as jnp
from jax import lax
from jax.experimental import pallas as pl
from jax.experimental.pallas import tpu as pltpu
from jax.sharding import PartitionSpec as P

LANES = 128
SUBLANES = 8
PARTS = 2
BITS = (4, 1, 2)
WALK = (0, 2, 1, 3)
REDUCERS = 2 * 2 * PARTS
MESH = pl.DeviceIdType.MESH


def cross_conj(first, second):
    row = []
    for k in range(3):
        a, b = (k + 1) % 3, (k + 2) % 3
        ar, ai = first[a]
        br, bi = first[b]
        cr, ci = second[a]
        dr, di = second[b]
        real = (ar * dr - ai * di) - (br * cr - bi * ci)
        imag = (br * ci + bi * cr) - (ar * di + ai * dr)
        row.append((real, imag))
    return row


def row_times(row, matrix):
    out = []
    for k in range(3):
        real = imag = None
        for m in range(3):
            ar, ai = row[m]
            br, bi = matrix[m][k]
            pr = ar * br - ai * bi
            pi = ar * bi + ai * br
            real = pr if real is None else real + pr
            imag = pi if imag is None else imag + pi
        out.append((real, imag))
    return out


def product_rows(load, slices):
    rows = [[load(r, c) for c in range(3)] for r in range(2)]
    for t in range(1, slices):
        matrix = [[load(2 * t + r, c) for c in range(3)] for r in range(2)]
        matrix.append(cross_conj(matrix[0], matrix[1]))
        rows = [row_times(row, matrix) for row in rows]
    return rows


def trace_of_product(left, right):
    right = right + [cross_conj(right[0], right[1])]
    real = imag = None
    for i in range(3):
        for j in range(3):
            ar, ai = left[i][j]
            br, bi = right[j][i]
            pr = ar * br - ai * bi
            pi = ar * bi + ai * br
            real = pr if real is None else real + pr
            imag = pi if imag is None else imag + pi
    return real / 3.0, imag / 3.0


def kernel(dims, split, x_ref, *refs):
    slices, planes, sites, gx_n, longest = dims
    count = len(split)
    refs = list(refs)

    def take(n):
        taken = refs[:n]
        del refs[:n]
        return taken

    loop_refs = take(count)
    (corr_ref,) = take(1)
    far_in = take(count)
    (near_pool,) = take(1)
    psend, precv, held, tr = take(count), take(count), take(count), take(count)
    gath = take(count)
    gram, part, in_sem, sent, r1, r2, r3, ready, beside = refs
    slab = planes // 2
    wide = planes * gx_n
    lane_tiles = gram.shape[0]
    ta = lax.axis_index("ta")
    gx = lax.axis_index("gx")
    other = 1 - ta
    half = sum(n for _, n in split)
    base = gx_n // 4
    step = gx_n // 2 // REDUCERS
    mine = (gx - base) // step
    is_home = jnp.logical_and(
        gx >= base,
        jnp.logical_and((gx - base) % step == 0, gx < base + REDUCERS * step),
    )
    is_reducer = jnp.logical_and(ta == 1, is_home)
    from_core, from_comp, from_part = (mine // bit % 2 for bit in BITS)
    from_part = 1 - from_part
    early = gx_n // 2 + gx_n // 4
    near_targets = gx_n // 4
    is_first = gx == 0
    is_slow = gx % 2 + gx // 2 % 2 + gx // 4 == 1

    half = sum(n for _, n in split)
    depth = near_pool.shape[0] // half
    near_in = [None] * count
    pairs = []
    place = 0
    for turn, p in enumerate(WALK):
        n = split[p][1]
        near_in[p] = near_pool.at[pl.ds(place * depth, n * depth)].reshape(
            depth // 3 // planes, 3, planes, n, 2, LANES
        )
        pairs += [(place, n)] if turn % 2 == 0 else []
        pairs[-1] = (pairs[-1][0], place + n - pairs[-1][0])
        place += n

    def home(h, q, core):
        return base + (core * BITS[0] + q * BITS[1] + (1 - h) * BITS[2]) * step

    def load_piece(order, p):
        owner = other if order == 0 else ta
        start, n = split[p]
        place = (far_in, near_in)[order][p]
        return pltpu.make_async_copy(
            x_ref.at[:, pl.ds(0, 2), :, :, pl.ds(owner * half + start, n)],
            place.reshape(slices, 2, *place.shape[1:]),
            in_sem.at[p if order == 0 else count + WALK.index(p) // 2],
        )

    def total(ref, semaphore):
        return pltpu.make_async_copy(ref, ref, semaphore)

    barrier = pltpu.get_barrier_semaphore()

    def arrive(semaphore, core, j):
        pl.semaphore_signal(semaphore, inc=1, device_id={"ta": core, "gx": j}, device_id_type=MESH)

    def greet():
        @pl.when(is_reducer)
        def _():
            for j in range(1, gx_n):

                @pl.when(j != gx)
                def _():
                    arrive(barrier, 1, j)

    greet()

    for order in range(2):
        for p in WALK:
            load_piece(order, p).start(priority=order)

    @pl.when(ta == 1)
    def _():
        arrive(barrier, 0, gx)

    @pl.when(is_first)
    def _():
        for h in range(PARTS):
            for q in range(2):
                arrive(barrier, 0, home(h, q, ta))

    @pl.when(ta == 0)
    def _():
        pl.semaphore_wait(barrier, jnp.where(is_home, 2, 1))
        arrive(beside, 1, gx)

        @pl.when(is_home)
        def _():
            arrive(ready.at[from_part * 2 + from_comp], from_core, 0)

    def clear():
        @pl.when(jnp.logical_and(ta == 1, jnp.logical_not(is_first)))
        def _():
            pl.semaphore_wait(barrier, jnp.where(is_home, REDUCERS - 1, REDUCERS))
            arrive(beside, 0, gx)

        @pl.when(jnp.logical_and(ta == 0, jnp.logical_not(is_first)))
        def _():
            pl.semaphore_wait(beside, 1)

    def rows_of(p):
        return planes * split[p][1]

    def begin(p, g):
        return jnp.minimum(g * SUBLANES, rows_of(p) - SUBLANES)

    def each_group(p, body):
        def run(g, carry):
            body(begin(p, g))
            return carry

        lax.fori_loop(0, -(-rows_of(p) // SUBLANES), run, 0)

    def loader(ref, rows, start):
        flat = ref.reshape(*ref.shape[:2], rows * 2, LANES)

        def load(i, c):
            return tuple(
                flat[i, c, pl.ds(2 * start + q, SUBLANES, stride=2), :] for q in range(2)
            )

        return load

    def flat_rows(ref):
        return ref.reshape(ref.shape[0], ref.shape[1] * 2, LANES)

    def swap(p):
        return pltpu.make_async_remote_copy(
            src_ref=psend[p],
            dst_ref=precv[p],
            send_sem=sent,
            recv_sem=r1.at[p],
            device_id={"ta": other, "gx": gx},
            device_id_type=MESH,
        )

    def do_far(p):
        load_piece(0, p).wait()

        def far(start, p=p):
            product = product_rows(loader(far_in[p], rows_of(p), start), slices)
            out = flat_rows(psend[p])
            for r in range(2):
                for k in range(3):
                    for q in range(2):
                        out[(r * 3 + k) * 2 + q, pl.ds(start, SUBLANES), :] = product[r][k][q]

        each_group(p, far)
        if p == 0:

            @pl.when(ta == 1)
            def _():
                pl.semaphore_wait(beside, 1)

        swap(p).start()

    def do_near(p):
        if WALK.index(p) % 2 == 0:
            first, length = pairs[WALK.index(p) // 2]
            total(near_pool.at[pl.ds(first * depth, length * depth)], in_sem.at[count + WALK.index(p) // 2]).wait()

        def near(start, p=p):
            product = product_rows(loader(near_in[p], rows_of(p), start), slices)
            product.append(cross_conj(product[0], product[1]))
            for r in range(3):
                for k in range(3):
                    for q in range(2):
                        held[p][(r * 3 + k) * 2 + q, pl.ds(start, SUBLANES), :] = product[r][k][q]

        each_group(p, near)

    def scatter(p, q, place):
        return pltpu.make_async_remote_copy(
            src_ref=tr[p].at[q],
            dst_ref=gath[p].at[gx],
            send_sem=sent,
            recv_sem=r2.at[jnp.where(gx < early, 0, 2) + p % 2],
            device_id={"ta": 1, "gx": place},
            device_id_type=MESH,
        )

    def hand_over(p, q):
        place = home(p // 2, q, ta)
        itself = jnp.logical_and(ta == 1, place == gx)

        @pl.when(jnp.logical_not(itself))
        def _():
            scatter(p, q, place).start()

        @pl.when(itself)
        def _():
            gath[p][gx] = tr[p][q]

    upper = jnp.where(gx < gx_n // 2, 1, 0)

    def do_trace(p):
        swap(p).wait_recv()

        def trace(start, p=p):
            theirs_ref = flat_rows(precv[p])

            def entry(ref, r, k):
                return tuple(ref[(r * 3 + k) * 2 + q, pl.ds(start, SUBLANES), :] for q in range(2))

            ours = [[entry(held[p], r, k) for k in range(3)] for r in range(3)]
            theirs = [[entry(theirs_ref, r, k) for k in range(3)] for r in range(2)]
            pair = trace_of_product(ours, theirs)
            flat_loop = loop_refs[p].reshape(rows_of(p) * 2, LANES)
            flat_tr = flat_rows(tr[p])
            for q in range(2):
                flat_loop[pl.ds(2 * start + q, SUBLANES, stride=2), :] = pair[q]
                flat_tr[q, pl.ds(start, SUBLANES), :] = pair[q]

        each_group(p, trace)
        at = WALK.index(p)
        def release(turn):
            hand_over(WALK[turn], upper)
            hand_over(WALK[turn], 1 - upper)

        @pl.when(jnp.logical_not(jnp.logical_or(is_first, is_slow)))
        def _():
            if at == 0:
                clear()
            release(at)

        if at >= 2:

            @pl.when(is_slow)
            def _():
                if at == 2:
                    clear()
                    release(0)
                    release(1)
                release(at)

    for work in (do_far, do_near, do_trace):
        for p in WALK:
            work(p)

    @pl.when(is_first)
    def _():
        for h in reversed(range(PARTS)):
            for q in range(2):
                pl.semaphore_wait(ready.at[h * 2 + q], 1)
                for k in range(2):
                    hand_over(h * 2 + k, q)

    def report(core, j, slot):
        return pltpu.make_async_remote_copy(
            src_ref=gram.at[:, pl.ds(j * slab, slab)],
            dst_ref=part.at[slot],
            send_sem=sent,
            recv_sem=r3,
            device_id={"ta": core, "gx": j},
            device_id_type=MESH,
        )

    flat_gram = gram.reshape(lane_tiles, wide, LANES)

    def contract(k, low, high, width):
        tiles = split[k][1]
        flat_gath = gath[k].reshape(gx_n * rows_of(k), LANES)
        tops, bottoms = [], []
        for i in range(tiles):
            values = flat_gath[pl.ds(i, width, stride=tiles), :]
            top = values.astype(jnp.bfloat16)
            tops.append(top)
            bottoms.append((values - top.astype(jnp.float32)).astype(jnp.bfloat16))
        top = jnp.concatenate(tops, axis=1)
        bottom = jnp.concatenate(bottoms, axis=1)

        def dot(a, b):
            return lax.dot_general(a, b, (((1,), (1,)), ((), ())), preferred_element_type=jnp.float32)

        return dot(top[low:high], top) + (dot(top[low:high], bottom) + dot(bottom[low:high], top))

    def place_rows(product, low, high, width):
        padding = lane_tiles * LANES - width
        if padding:
            product = jnp.concatenate([product, jnp.zeros((high - low, padding), jnp.float32)], axis=1)
        for i in range(lane_tiles):
            flat_gram[i, low:high] = product[:, i * LANES : (i + 1) * LANES]

    def tell(j, carry):
        for core in range(2):

            @pl.when(jnp.logical_or(core != ta, j != gx))
            def _():
                report(core, j, mine).start()

        return carry

    first_rows = planes * near_targets

    def reduce_part(h):
        pieces = (2 * h, 2 * h + 1)
        products = []
        for k, p in enumerate(pieces):
            @pl.when(from_core == 0)
            def _():
                total(gath[p].at[pl.ds(0, early)], r2.at[k]).wait()

            @pl.when(from_core == 1)
            def _():
                total(gath[p].at[pl.ds(0, early - 1)], r2.at[k]).wait()

            products.append(contract(p, 0, first_rows, planes * early))
        place_rows(products[0] + products[1], 0, first_rows, planes * early)
        lax.fori_loop(0, near_targets, tell, 0)
        products = []
        for k, p in enumerate(pieces):
            total(gath[p].at[pl.ds(0, gx_n - early)], r2.at[2 + k]).wait()
            products.append(contract(p, first_rows, wide, wide))
        place_rows(products[0] + products[1], first_rows, wide, wide)
        lax.fori_loop(near_targets, gx_n, tell, 0)

    for h in range(PARTS):

        @pl.when(jnp.logical_and(is_reducer, from_part == h))
        def _():
            reduce_part(h)

    @pl.when(is_reducer)
    def _():
        part[mine] = gram[:, pl.ds(gx * slab, slab)]
        total(part.at[pl.ds(0, REDUCERS - 1)], r3).wait()

    @pl.when(jnp.logical_not(is_reducer))
    def _():
        total(part, r3).wait()

    flat_part = part.reshape(REDUCERS, lane_tiles, planes, LANES)
    chunks = []
    for i in range(lane_tiles):
        chunk = flat_part[0, i]
        for slot in range(1, REDUCERS):
            chunk = chunk + flat_part[slot, i]
        chunks.append(chunk)
    summed = chunks[0] if lane_tiles == 1 else jnp.concatenate(chunks, axis=1)
    extra = -planes % SUBLANES
    if extra:
        summed = jnp.concatenate([summed, jnp.zeros((extra, summed.shape[1]), jnp.float32)], axis=0)
    corr_ref[...] = summed

    def drain(length):
        while length:
            some = min(length, near_pool.shape[0])
            total(near_pool.at[pl.ds(0, some)], sent).wait()
            length -= some

    shared = 7 * planes * half
    reports = (2 * gx_n - 1) * slab * lane_tiles
    inside = jnp.logical_and(is_reducer, from_core == 1)

    @pl.when(jnp.logical_not(is_reducer))
    def _():
        drain(shared)

    @pl.when(jnp.logical_and(is_reducer, from_core == 0))
    def _():
        drain(shared + reports)

    for h in range(PARTS):

        @pl.when(jnp.logical_and(inside, from_part == h))
        def _():
            drain(shared + reports - (rows_of(2 * h) + rows_of(2 * h + 1)) // 2)


def place_outputs(dims, split, *refs):
    planes, sites, gx_n, longest = dims[1:]
    wide = planes * gx_n
    count = len(split)
    loop_in, (total_ref, loop_out, corr_out, corr, semaphores) = refs[:count], refs[count:]
    gx = lax.axis_index("gx")
    copies = [
        pltpu.make_async_copy(loop_in[p], loop_out.at[:, pl.ds(start, n)], semaphores.at[p])
        for p, (start, n) in enumerate(split)
    ]
    for copy in copies:
        copy.start()
    summed = total_ref[...]
    width = summed.shape[1]
    row_index = lax.broadcasted_iota(jnp.int32, summed.shape, 0)
    column = lax.broadcasted_iota(jnp.int32, summed.shape, 1)
    answer = jnp.zeros(summed.shape, jnp.float32)
    for i in range(planes):
        start = gx * planes + i
        ahead = pltpu.roll(summed, (width - start) % width, 1)
        if width == wide:
            value = ahead
        else:
            around = pltpu.roll(summed, (width + wide - start) % width, 1)
            value = jnp.where(column + start < wide, ahead, around)
        answer = jnp.where(row_index == i, value, answer)
    corr[...] = answer[0:planes, 0 : longest + 1] / sites
    last = pltpu.make_async_copy(corr, corr_out, semaphores.at[count])
    last.start()
    for copy in copies:
        copy.wait()
    last.wait()


def per_device(gx_n, time_links):
    slices, _, _, _, planes, sites = time_links.shape
    blocks = sites // LANES
    held = time_links.transpose(0, 2, 3, 4, 1, 5)
    held = held.reshape(slices, 3, 3, planes, 2, blocks, LANES).swapaxes(4, 5)
    half = blocks // 2
    less = half // PARTS
    split = []
    for start, tiles in ((0, less), (less, half - less)):
        lead = tiles - tiles // 2
        split += [(start, lead), (start + lead, tiles - lead)]
    longest = planes * (gx_n // 2)
    wide = planes * gx_n
    lane_tiles = -(-wide // LANES)
    dims = (slices, planes, sites, gx_n, longest)
    dma = pltpu.SemaphoreType.DMA
    regular = pltpu.SemaphoreType.REGULAR
    f32 = jnp.float32
    count = len(split)
    links = [
        pltpu.VMEM((2 * slices, 3, planes, n, 2, LANES), f32)
        for _, n in split
    ]
    links.append(pltpu.VMEM((2 * slices * 3 * planes * half, 2, LANES), f32))
    swaps = [pltpu.VMEM((12, planes * n // 2, 2, LANES), f32) for _, n in split]
    scratch = links + swaps + swaps
    scratch += [pltpu.VMEM((18, planes * n, LANES), f32) for _, n in split]
    scratch += [pltpu.VMEM((2, planes * n // 2, 2, LANES), f32) for _, n in split]
    scratch += [pltpu.VMEM((gx_n, planes * n // 2, 2, LANES), f32) for _, n in split]
    scratch += [
        pltpu.VMEM((lane_tiles, wide // 2, 2, LANES), f32),
        pltpu.VMEM((REDUCERS, lane_tiles, planes // 2, 2, LANES), f32),
        dma((count + count // 2,)),
        dma,
        dma((count,)),
        dma((4,)),
        dma,
        regular((2 * PARTS,)),
        regular,
    ]
    in_vmem = pl.BlockSpec(memory_space=pltpu.VMEM)
    results = pl.pallas_call(
        functools.partial(kernel, dims, split),
        out_shape=[pltpu.VMEM((planes, n, 2, LANES), f32) for _, n in split]
        + [pltpu.VMEM((-(-planes // SUBLANES) * SUBLANES, lane_tiles * LANES), f32)],
        in_specs=[pl.BlockSpec(memory_space=pl.ANY)],
        out_specs=[in_vmem] * (count + 1),
        scratch_shapes=scratch,
        compiler_params=pltpu.CompilerParams(collective_id=0, has_side_effects=True),
    )(held)
    results = [pltpu.with_memory_space_constraint(r, pltpu.VMEM) for r in results]
    loops, correlator = pl.pallas_call(
        functools.partial(place_outputs, dims, split),
        out_shape=(
            jax.ShapeDtypeStruct((planes, half, 2, LANES), f32),
            jax.ShapeDtypeStruct((planes, longest + 1), f32),
        ),
        in_specs=[in_vmem] * (count + 1),
        out_specs=(pl.BlockSpec(memory_space=pl.ANY),) * 2,
        scratch_shapes=[pltpu.VMEM((planes, longest + 1), f32), dma((count + 1,))],
    )(*results)
    return loops.swapaxes(1, 2).reshape(planes, 2, sites // 2), correlator


def solution(mesh):
    in_specs = (P("ta", None, None, None, "gx", None),)
    out_specs = (P("gx", None, "ta"), P("gx", None))
    return jax.shard_map(
        functools.partial(per_device, mesh.shape["gx"]),
        mesh=mesh,
        in_specs=in_specs,
        out_specs=out_specs,
        check_vma=False,
    )
```

```python
import functools

import jax
import jax.numpy as jnp
from jax import lax
from jax.experimental import pallas as pl
from jax.experimental.pallas import tpu as pltpu
from jax.sharding import PartitionSpec as P

LANES = 128
SUBLANES = 8
PARTS = 2
BITS = (4, 1, 2)
WALK = (0, 2, 1, 3)
REDUCERS = 2 * 2 * PARTS
MESH = pl.DeviceIdType.MESH


def cross_conj(first, second):
    row = []
    for k in range(3):
        a, b = (k + 1) % 3, (k + 2) % 3
        ar, ai = first[a]
        br, bi = first[b]
        cr, ci = second[a]
        dr, di = second[b]
        real = (ar * dr - ai * di) - (br * cr - bi * ci)
        imag = (br * ci + bi * cr) - (ar * di + ai * dr)
        row.append((real, imag))
    return row


def row_times(row, matrix):
    out = []
    for k in range(3):
        real = imag = None
        for m in range(3):
            ar, ai = row[m]
            br, bi = matrix[m][k]
            pr = ar * br - ai * bi
            pi = ar * bi + ai * br
            real = pr if real is None else real + pr
            imag = pi if imag is None else imag + pi
        out.append((real, imag))
    return out


def product_rows(load, slices):
    rows = [[load(r, c) for c in range(3)] for r in range(2)]
    for t in range(1, slices):
        matrix = [[load(2 * t + r, c) for c in range(3)] for r in range(2)]
        matrix.append(cross_conj(matrix[0], matrix[1]))
        rows = [row_times(row, matrix) for row in rows]
    return rows


def trace_of_product(left, right):
    right = right + [cross_conj(right[0], right[1])]
    real = imag = None
    for i in range(3):
        for j in range(3):
            ar, ai = left[i][j]
            br, bi = right[j][i]
            pr = ar * br - ai * bi
            pi = ar * bi + ai * br
            real = pr if real is None else real + pr
            imag = pi if imag is None else imag + pi
    return real / 3.0, imag / 3.0


def kernel(dims, split, x_ref, *refs):
    slices, planes, sites, gx_n, longest = dims
    count = len(split)
    refs = list(refs)

    def take(n):
        taken = refs[:n]
        del refs[:n]
        return taken

    loop_refs = take(count)
    (corr_ref,) = take(1)
    far_in = take(count)
    (near_pool,) = take(1)
    psend, precv, held, tr = take(count), take(count), take(count), take(count)
    gath = take(count)
    gram, part, in_sem, sent, r1, r2, r3, ready, beside = refs
    slab = planes // 2
    wide = planes * gx_n
    lane_tiles = gram.shape[0]
    ta = lax.axis_index("ta")
    gx = lax.axis_index("gx")
    other = 1 - ta
    half = sum(n for _, n in split)
    base = gx_n // 4
    step = gx_n // 2 // REDUCERS
    mine = (gx - base) // step
    is_home = jnp.logical_and(
        gx >= base,
        jnp.logical_and((gx - base) % step == 0, gx < base + REDUCERS * step),
    )
    is_reducer = jnp.logical_and(ta == 1, is_home)
    from_core, from_comp, from_part = (mine // bit % 2 for bit in BITS)
    from_part = 1 - from_part
    early = gx_n // 2 + gx_n // 4
    near_targets = gx_n // 4
    is_first = gx == 0
    is_slow = gx % 2 + gx // 2 % 2 + gx // 4 == 1

    depth = near_pool.shape[0] // half
    near_in = [None] * count
    pairs = []
    place = 0
    for turn, p in enumerate(WALK):
        n = split[p][1]
        near_in[p] = near_pool.at[pl.ds(place * depth, n * depth)].reshape(
            depth // 3 // planes, 3, planes, n, 2, LANES
        )
        pairs += [(place, n)] if turn % 2 == 0 else []
        pairs[-1] = (pairs[-1][0], place + n - pairs[-1][0])
        place += n

    def home(h, q, core):
        return base + (core * BITS[0] + q * BITS[1] + (1 - h) * BITS[2]) * step

    def load_piece(order, p):
        owner = other if order == 0 else ta
        start, n = split[p]
        place = (far_in, near_in)[order][p]
        return pltpu.make_async_copy(
            x_ref.at[:, pl.ds(0, 2), :, :, pl.ds(owner * half + start, n)],
            place.reshape(slices, 2, *place.shape[1:]),
            in_sem.at[p if order == 0 else count + WALK.index(p) // 2],
        )

    def total(ref, semaphore):
        return pltpu.make_async_copy(ref, ref, semaphore)

    barrier = pltpu.get_barrier_semaphore()

    def arrive(semaphore, core, j):
        pl.semaphore_signal(semaphore, inc=1, device_id={"ta": core, "gx": j}, device_id_type=MESH)

    def greet():
        @pl.when(is_reducer)
        def _():
            for j in range(1, gx_n):

                @pl.when(j != gx)
                def _():
                    arrive(barrier, 1, j)

    greet()

    for order in range(2):
        for p in WALK:
            load_piece(order, p).start(priority=order)

    @pl.when(ta == 1)
    def _():
        arrive(barrier, 0, gx)

    @pl.when(is_first)
    def _():
        for h in range(PARTS):
            for q in range(2):
                arrive(barrier, 0, home(h, q, ta))

    @pl.when(ta == 0)
    def _():
        pl.semaphore_wait(barrier, jnp.where(is_home, 2, 1))
        arrive(beside, 1, gx)

        @pl.when(is_home)
        def _():
            arrive(ready.at[from_part * 2 + from_comp], from_core, 0)

    def clear():
        @pl.when(jnp.logical_and(ta == 1, jnp.logical_not(is_first)))
        def _():
            pl.semaphore_wait(barrier, jnp.where(is_home, REDUCERS - 1, REDUCERS))
            arrive(beside, 0, gx)

        @pl.when(jnp.logical_and(ta == 0, jnp.logical_not(is_first)))
        def _():
            pl.semaphore_wait(beside, 1)

    def rows_of(p):
        return planes * split[p][1]

    def begin(p, g):
        return jnp.minimum(g * SUBLANES, rows_of(p) - SUBLANES)

    def each_group(p, body):
        def run(g, carry):
            body(begin(p, g))
            return carry

        lax.fori_loop(0, -(-rows_of(p) // SUBLANES), run, 0, unroll=True)

    def loader(ref, rows, start):
        flat = ref.reshape(*ref.shape[:2], rows * 2, LANES)

        def load(i, c):
            return tuple(
                flat[i, c, pl.ds(2 * start + q, SUBLANES, stride=2), :] for q in range(2)
            )

        return load

    def flat_rows(ref):
        return ref.reshape(ref.shape[0], ref.shape[1] * 2, LANES)

    def swap(p):
        return pltpu.make_async_remote_copy(
            src_ref=psend[p],
            dst_ref=precv[p],
            send_sem=sent,
            recv_sem=r1.at[p],
            device_id={"ta": other, "gx": gx},
            device_id_type=MESH,
        )

    def do_far(p):
        load_piece(0, p).wait()

        def far(start, p=p):
            product = product_rows(loader(far_in[p], rows_of(p), start), slices)
            out = flat_rows(psend[p])
            for r in range(2):
                for k in range(3):
                    for q in range(2):
                        out[(r * 3 + k) * 2 + q, pl.ds(start, SUBLANES), :] = product[r][k][q]

        each_group(p, far)
        if p == 0:

            @pl.when(ta == 1)
            def _():
                pl.semaphore_wait(beside, 1)

        swap(p).start()

    def do_near(p):
        if WALK.index(p) % 2 == 0:
            first, length = pairs[WALK.index(p) // 2]
            total(near_pool.at[pl.ds(first * depth, length * depth)], in_sem.at[count + WALK.index(p) // 2]).wait()

        def near(start, p=p):
            product = product_rows(loader(near_in[p], rows_of(p), start), slices)
            product.append(cross_conj(product[0], product[1]))
            for r in range(3):
                for k in range(3):
                    for q in range(2):
                        held[p][(r * 3 + k) * 2 + q, pl.ds(start, SUBLANES), :] = product[r][k][q]

        each_group(p, near)

    def scatter(p, q, place):
        return pltpu.make_async_remote_copy(
            src_ref=tr[p].at[q],
            dst_ref=gath[p].at[gx],
            send_sem=sent,
            recv_sem=r2.at[jnp.where(gx < early, 0, 2) + p % 2],
            device_id={"ta": 1, "gx": place},
            device_id_type=MESH,
        )

    def hand_over(p, q):
        place = home(p // 2, q, ta)
        itself = jnp.logical_and(ta == 1, place == gx)

        @pl.when(jnp.logical_not(itself))
        def _():
            scatter(p, q, place).start()

        @pl.when(itself)
        def _():
            gath[p][gx] = tr[p][q]

    upper = jnp.where(gx < gx_n // 2, 1, 0)

    def do_trace(p):
        swap(p).wait_recv()

        def trace(start, p=p):
            theirs_ref = flat_rows(precv[p])

            def entry(ref, r, k):
                return tuple(ref[(r * 3 + k) * 2 + q, pl.ds(start, SUBLANES), :] for q in range(2))

            ours = [[entry(held[p], r, k) for k in range(3)] for r in range(3)]
            theirs = [[entry(theirs_ref, r, k) for k in range(3)] for r in range(2)]
            pair = trace_of_product(ours, theirs)
            flat_loop = loop_refs[p].reshape(rows_of(p) * 2, LANES)
            flat_tr = flat_rows(tr[p])
            for q in range(2):
                flat_loop[pl.ds(2 * start + q, SUBLANES, stride=2), :] = pair[q]
                flat_tr[q, pl.ds(start, SUBLANES), :] = pair[q]

        each_group(p, trace)
        at = WALK.index(p)

        def release(turn):
            hand_over(WALK[turn], upper)
            hand_over(WALK[turn], 1 - upper)

        @pl.when(jnp.logical_not(jnp.logical_or(is_first, is_slow)))
        def _():
            if at == 0:
                clear()
            release(at)

        if at >= 2:

            @pl.when(is_slow)
            def _():
                if at == 2:
                    clear()
                    release(0)
                    release(1)
                release(at)

    for work in (do_far, do_near, do_trace):
        for p in WALK:
            work(p)

    @pl.when(is_first)
    def _():
        for h in reversed(range(PARTS)):
            for q in range(2):
                pl.semaphore_wait(ready.at[h * 2 + q], 1)
                for k in range(2):
                    hand_over(h * 2 + k, q)

    def report(core, j, slot):
        return pltpu.make_async_remote_copy(
            src_ref=gram.at[:, pl.ds(j * slab, slab)],
            dst_ref=part.at[slot],
            send_sem=sent,
            recv_sem=r3,
            device_id={"ta": core, "gx": j},
            device_id_type=MESH,
        )

    flat_gram = gram.reshape(lane_tiles, wide, LANES)

    def contract(k, low, high, width):
        tiles = split[k][1]
        flat_gath = gath[k].reshape(gx_n * rows_of(k), LANES)
        tops, bottoms = [], []
        for i in range(tiles):
            values = flat_gath[pl.ds(i, width, stride=tiles), :]
            top = values.astype(jnp.bfloat16)
            tops.append(top)
            bottoms.append((values - top.astype(jnp.float32)).astype(jnp.bfloat16))
        top = jnp.concatenate(tops, axis=1)
        bottom = jnp.concatenate(bottoms, axis=1)

        def dot(a, b):
            return lax.dot_general(a, b, (((1,), (1,)), ((), ())), preferred_element_type=jnp.float32)

        return dot(top[low:high], top) + (dot(top[low:high], bottom) + dot(bottom[low:high], top))

    def place_rows(product, low, high, width):
        padding = lane_tiles * LANES - width
        if padding:
            product = jnp.concatenate([product, jnp.zeros((high - low, padding), jnp.float32)], axis=1)
        for i in range(lane_tiles):
            flat_gram[i, low:high] = product[:, i * LANES : (i + 1) * LANES]

    def tell(j, carry):
        for core in range(2):

            @pl.when(jnp.logical_or(core != ta, j != gx))
            def _():
                report(core, j, mine).start()

        return carry

    first_rows = planes * near_targets

    def reduce_part(h):
        pieces = (2 * h, 2 * h + 1)
        products = []
        for k, p in enumerate(pieces):
            @pl.when(from_core == 0)
            def _():
                total(gath[p].at[pl.ds(0, early)], r2.at[k]).wait()

            @pl.when(from_core == 1)
            def _():
                total(gath[p].at[pl.ds(0, early - 1)], r2.at[k]).wait()

            products.append(contract(p, 0, first_rows, planes * early))
        place_rows(products[0] + products[1], 0, first_rows, planes * early)
        lax.fori_loop(0, near_targets, tell, 0)
        products = []
        for k, p in enumerate(pieces):
            total(gath[p].at[pl.ds(0, gx_n - early)], r2.at[2 + k]).wait()
            products.append(contract(p, first_rows, wide, wide))
        place_rows(products[0] + products[1], first_rows, wide, wide)
        lax.fori_loop(near_targets, gx_n, tell, 0)

    for h in range(PARTS):

        @pl.when(jnp.logical_and(is_reducer, from_part == h))
        def _():
            reduce_part(h)

    @pl.when(is_reducer)
    def _():
        part[mine] = gram[:, pl.ds(gx * slab, slab)]
        total(part.at[pl.ds(0, REDUCERS - 1)], r3).wait()

    @pl.when(jnp.logical_not(is_reducer))
    def _():
        total(part, r3).wait()

    flat_part = part.reshape(REDUCERS, lane_tiles, planes, LANES)
    chunks = []
    for i in range(lane_tiles):
        chunk = flat_part[0, i]
        for slot in range(1, REDUCERS):
            chunk = chunk + flat_part[slot, i]
        chunks.append(chunk)
    summed = chunks[0] if lane_tiles == 1 else jnp.concatenate(chunks, axis=1)
    extra = -planes % SUBLANES
    if extra:
        summed = jnp.concatenate([summed, jnp.zeros((extra, summed.shape[1]), jnp.float32)], axis=0)
    corr_ref[...] = summed

    def drain(length):
        while length:
            some = min(length, near_pool.shape[0])
            total(near_pool.at[pl.ds(0, some)], sent).wait()
            length -= some

    shared = 7 * planes * half
    reports = (2 * gx_n - 1) * slab * lane_tiles
    inside = jnp.logical_and(is_reducer, from_core == 1)

    @pl.when(jnp.logical_not(is_reducer))
    def _():
        drain(shared)

    @pl.when(jnp.logical_and(is_reducer, from_core == 0))
    def _():
        drain(shared + reports)

    for h in range(PARTS):

        @pl.when(jnp.logical_and(inside, from_part == h))
        def _():
            drain(shared + reports - (rows_of(2 * h) + rows_of(2 * h + 1)) // 2)


def place_outputs(dims, split, *refs):
    planes, sites, gx_n, longest = dims[1:]
    wide = planes * gx_n
    count = len(split)
    loop_in, (total_ref, loop_out, corr_out, corr, semaphores) = refs[:count], refs[count:]
    gx = lax.axis_index("gx")
    copies = [
        pltpu.make_async_copy(loop_in[p], loop_out.at[:, pl.ds(start, n)], semaphores.at[p])
        for p, (start, n) in enumerate(split)
    ]
    for copy in copies:
        copy.start()
    summed = total_ref[...]
    width = summed.shape[1]
    row_index = lax.broadcasted_iota(jnp.int32, summed.shape, 0)
    column = lax.broadcasted_iota(jnp.int32, summed.shape, 1)
    answer = jnp.zeros(summed.shape, jnp.float32)
    for i in range(planes):
        start = gx * planes + i
        ahead = pltpu.roll(summed, (width - start) % width, 1)
        if width == wide:
            value = ahead
        else:
            around = pltpu.roll(summed, (width + wide - start) % width, 1)
            value = jnp.where(column + start < wide, ahead, around)
        answer = jnp.where(row_index == i, value, answer)
    corr[...] = answer[0:planes, 0 : longest + 1] / sites
    last = pltpu.make_async_copy(corr, corr_out, semaphores.at[count])
    last.start()
    for copy in copies:
        copy.wait()
    last.wait()


def per_device(gx_n, time_links):
    slices, _, _, _, planes, sites = time_links.shape
    blocks = sites // LANES
    held = time_links.transpose(0, 2, 3, 4, 1, 5)
    held = held.reshape(slices, 3, 3, planes, 2, blocks, LANES).swapaxes(4, 5)
    half = blocks // 2
    less = half // PARTS
    split = []
    for start, tiles in ((0, less), (less, half - less)):
        lead = tiles - tiles // 2
        split += [(start, lead), (start + lead, tiles - lead)]
    longest = planes * (gx_n // 2)
    wide = planes * gx_n
    lane_tiles = -(-wide // LANES)
    dims = (slices, planes, sites, gx_n, longest)
    dma = pltpu.SemaphoreType.DMA
    regular = pltpu.SemaphoreType.REGULAR
    f32 = jnp.float32
    count = len(split)
    links = [
        pltpu.VMEM((2 * slices, 3, planes, n, 2, LANES), f32)
        for _, n in split
    ]
    links.append(pltpu.VMEM((2 * slices * 3 * planes * half, 2, LANES), f32))
    swaps = [pltpu.VMEM((12, planes * n // 2, 2, LANES), f32) for _, n in split]
    scratch = links + swaps + swaps
    scratch += [pltpu.VMEM((18, planes * n, LANES), f32) for _, n in split]
    scratch += [pltpu.VMEM((2, planes * n // 2, 2, LANES), f32) for _, n in split]
    scratch += [pltpu.VMEM((gx_n, planes * n // 2, 2, LANES), f32) for _, n in split]
    scratch += [
        pltpu.VMEM((lane_tiles, wide // 2, 2, LANES), f32),
        pltpu.VMEM((REDUCERS, lane_tiles, planes // 2, 2, LANES), f32),
        dma((count + count // 2,)),
        dma,
        dma((count,)),
        dma((4,)),
        dma,
        regular((2 * PARTS,)),
        regular,
    ]
    in_vmem = pl.BlockSpec(memory_space=pltpu.VMEM)
    results = pl.pallas_call(
        functools.partial(kernel, dims, split),
        out_shape=[pltpu.VMEM((planes, n, 2, LANES), f32) for _, n in split]
        + [pltpu.VMEM((-(-planes // SUBLANES) * SUBLANES, lane_tiles * LANES), f32)],
        in_specs=[pl.BlockSpec(memory_space=pl.ANY)],
        out_specs=[in_vmem] * (count + 1),
        scratch_shapes=scratch,
        compiler_params=pltpu.CompilerParams(collective_id=0, has_side_effects=True),
    )(held)
    results = [pltpu.with_memory_space_constraint(r, pltpu.VMEM) for r in results]
    loops, correlator = pl.pallas_call(
        functools.partial(place_outputs, dims, split),
        out_shape=(
            jax.ShapeDtypeStruct((planes, half, 2, LANES), f32),
            jax.ShapeDtypeStruct((planes, longest + 1), f32),
        ),
        in_specs=[in_vmem] * (count + 1),
        out_specs=(pl.BlockSpec(memory_space=pl.ANY),) * 2,
        scratch_shapes=[pltpu.VMEM((planes, longest + 1), f32), dma((count + 1,))],
    )(*results)
    return loops.swapaxes(1, 2).reshape(planes, 2, sites // 2), correlator


def solution(mesh):
    in_specs = (P("ta", None, None, None, "gx", None),)
    out_specs = (P("gx", None, "ta"), P("gx", None))
    return jax.shard_map(
        functools.partial(per_device, mesh.shape["gx"]),
        mesh=mesh,
        in_specs=in_specs,
        out_specs=out_specs,
        check_vma=False,
    )
```
